32 devices in a mesh: rows: 8 (over z, x), cols: 4 (over y, core).
Axes of the slice: x: 2, y: 2, z: 4, core: 2. Of those that a mesh axis runs over, the one named last changes fastest.
Arguments:
- leading_scene_data: float32 [2, 1024, 8192], P(None, 'rows', 'cols'), may hold values from -12 to 12, as said below
- trailing_scene_data: float32 [2, 1024, 8192], P(None, 'rows', 'cols'), may hold values from -20 to 20, as said below
- shared_usable_flags: int32 [1024, 8192], P('rows', 'cols'), may hold values 0 or 1
- sweep_of_each_line: int32 [1024], P('rows'), may hold values from 0 to 15, never falling along the last dimension, each value on 1 to 128 neighbouring positions
Outputs:
- deramped: float32 [2, 1024, 8192], P(None, 'rows', 'cols')
- coherence: float32 [1024, 8192], P('rows', 'cols')
The draws below stay inside these ranges and needn't reach their ends.
Inputs may be any that keep to these rules, and one draw needn't show every extreme that they name: `leading_scene_data`: first scene's parts lie in [-12, 12]. `trailing_scene_data`: second scene's parts lie in [-20, 20]; it is the first scene rotated by a smooth phase plus independent noise. `sweep_of_each_line`: burst ids never fall along the rows; each burst holds 1 to 128 rows, one exactly that many.
All inputs are finite; a program needn't handle non-finite values.
Results may differ from the reference program's by a relative error of at most 0.0003.
Values sent between devices are 32-bit elements.
A program may use at most 64 MiB of HBM per device.

```python
import math
import jax
import jax.numpy as jnp
import numpy as np
from jax import lax

WIN_R = 32
WIN_C = 8
SWEEP_TALLY = 16
SCENE_LINES = 1024
NC = 8192


def scene_primary(key):
    planes = jnp.clip(jax.random.normal(jax.random.fold_in(key, 11), (2, SCENE_LINES, NC), jnp.float32), -6.0, 6.0)
    return planes


def draw_leading_scene_data(key, part):
    return scene_primary(key)


def draw_trailing_scene_data(key, part):
    planes = scene_primary(key)
    speckle = jnp.clip(jax.random.normal(jax.random.fold_in(key, 12), (2, SCENE_LINES, NC), jnp.float32), -6.0, 6.0)
    slopes = jax.random.uniform(jax.random.fold_in(key, 13), (2,), jnp.float32)
    across_slope_term = 2.0 + 2.0 * slopes[0]
    along_slope_term = 1.5 + 1.5 * slopes[1]
    across_coordinate = (jnp.arange(NC, dtype=jnp.float32) + 0.5) / NC
    along_coordinate = (jnp.arange(SCENE_LINES, dtype=jnp.float32) + 0.5) / SCENE_LINES
    planar_angle_fit = across_slope_term * across_coordinate[None, :] + along_slope_term * SWEEP_TALLY * along_coordinate[:, None]
    cos_part = jnp.cos(planar_angle_fit)
    sine_part = jnp.sin(planar_angle_fit)
    real_b = 0.8 * (planes[0] * cos_part + planes[1] * sine_part) + 0.6 * speckle[0]
    imag_b = 0.8 * (planes[1] * cos_part - planes[0] * sine_part) + 0.6 * speckle[1]
    return jnp.stack([real_b, imag_b])


def touch_ends(array, stream_key, smallest, high):
    spot = [jax.random.randint(jax.random.fold_in(stream_key, axis), (), 0, length) for axis, length in enumerate(array.shape)]
    longest = array.shape.index(max(array.shape))
    neighbour = spot[:longest] + [(spot[longest] + 1) % array.shape[longest]] + spot[longest + 1:]
    return array.at[tuple(spot)].set(smallest).at[tuple(neighbour)].set(high)


def profile(count, total, bound, slope):
    weights = [(1 << 20) // math.isqrt(grade ** slope) + 1 for grade in range(2, count + 1)]
    spare, holding = total - bound - (count - 1), [1] * (count - 1)
    while spare > 0:
        candidates = [i for i in range(count - 1) if holding[i] < bound]
        whole, left = sum([weights[i] for i in candidates]), spare
        for i in candidates:
            addition = min(bound - holding[i], max(1, left * weights[i] // whole), spare)
            holding[i] = holding[i] + addition
            spare = spare - addition
    return np.array([bound] + holding)


def ragged(key, count, total, most, skew):
    if count == 2:
        one = jax.random.randint(key, (), max(1, total - most), min(most, total - 1) + 1)
        return jnp.stack([one, total - one])
    tallies = jnp.asarray(profile(count, total, most, skew), jnp.int32)
    couples = (count - 1) // 2
    source_of, taker = tallies[1:1 + 2 * couples:2], tallies[2:2 + 2 * couples:2]
    slack = jnp.minimum(source_of - 1, most - taker)
    passed = jax.random.randint(jax.random.fold_in(key, 1), (couples,), 0, 1 << 20) % (slack + 1)
    tallies = tallies.at[1:1 + 2 * couples:2].set(source_of - passed).at[2:2 + 2 * couples:2].set(taker + passed)
    return tallies[jax.random.permutation(jax.random.fold_in(key, 2), count)]


def setup_inputs(seed: int = 0) -> dict:
    keys = jax.random.split(jax.random.key(seed), 5)
    leading_scene_data = draw_leading_scene_data(jax.random.fold_in(keys[4], 71), 0)
    trailing_scene_data = draw_trailing_scene_data(jax.random.fold_in(keys[4], 71), 0)
    shared_usable_flags = touch_ends((jax.random.randint(keys[2], (SCENE_LINES, NC), 0, 8) < 7).astype(jnp.int32), jax.random.fold_in(keys[2], 1), 0, 1)
    sweep_of_each_line = jnp.searchsorted(jnp.cumsum(ragged(keys[3], SWEEP_TALLY, SCENE_LINES, 2 * SCENE_LINES // SWEEP_TALLY, 1)), jnp.arange(SCENE_LINES), side="right").astype(jnp.int32)
    return {"leading_scene_data": leading_scene_data, "trailing_scene_data": trailing_scene_data, "shared_usable_flags": shared_usable_flags, "sweep_of_each_line": sweep_of_each_line}


largest_value = lax.Precision.HIGHEST

def box_filter(plane):
    zero_value = jnp.zeros((), plane.dtype)
    return lax.reduce_window(plane, zero_value, lax.add, (WIN_R, WIN_C), (1, 1), ((WIN_R // 2, WIN_R // 2 - 1), (WIN_C // 2, WIN_C // 2 - 1)))

def sweep_aggregates(sweep_membership, line_aggregates):
    return jnp.dot(sweep_membership.T, line_aggregates, precision=largest_value)

def solve_ramps(pixel_count, moment_cc, moment_cr, moment_rr, sums):
    ridge_term = 0.001 * pixel_count + 1.0
    diag_col = moment_cc + ridge_term
    diag_row = moment_rr + ridge_term
    determinant = diag_col * diag_row - moment_cr * moment_cr
    base_part = sums[:, 0:2] / (pixel_count + ridge_term)[:, None]
    col_slope = (diag_row[:, None] * sums[:, 2:4] - moment_cr[:, None] * sums[:, 4:6]) / determinant[:, None]
    row_slope = (diag_col[:, None] * sums[:, 4:6] - moment_cr[:, None] * sums[:, 2:4]) / determinant[:, None]
    return jnp.concatenate([base_part, col_slope, row_slope], 1)

def reference(leading_scene_data, trailing_scene_data, shared_usable_flags, sweep_of_each_line):
    weight = shared_usable_flags.astype(jnp.float32)
    real_a = leading_scene_data[0] * weight
    imag_a = leading_scene_data[1] * weight
    real_b = trailing_scene_data[0] * weight
    imag_b = trailing_scene_data[1] * weight
    boxed_real = box_filter(real_a * real_b + imag_a * imag_b)
    boxed_imag = box_filter(imag_a * real_b - real_a * imag_b)
    boxed_pa = box_filter(real_a * real_a + imag_a * imag_a)
    boxed_pb = box_filter(real_b * real_b + imag_b * imag_b)
    normaliser = jnp.sqrt((boxed_pa + 1.0) * (boxed_pb + 1.0))
    coh_real = boxed_real / normaliser
    coh_imag = boxed_imag / normaliser
    coherence = jnp.sqrt(coh_real * coh_real + coh_imag * coh_imag)
    across_coordinate = (jnp.arange(NC, dtype=jnp.float32) + 0.5) * (2.0 / NC) - 1.0
    along_coordinate = (jnp.arange(SCENE_LINES, dtype=jnp.float32) + 0.5) * (2.0 / SCENE_LINES) - 1.0
    sweep_membership = (sweep_of_each_line[:, None] == jnp.arange(SWEEP_TALLY, dtype=jnp.int32)[None, :]).astype(jnp.float32)
    line_usable_tally = lax.optimization_barrier(jnp.sum(weight, 1))
    along_across_moment = lax.optimization_barrier(jnp.sum(weight * across_coordinate[None, :], 1))
    recentered_aggregates = sweep_aggregates(sweep_membership, jnp.stack([line_usable_tally, along_across_moment, along_coordinate * line_usable_tally], 1))
    pixel_count = recentered_aggregates[:, 0]
    floored = jnp.maximum(pixel_count, 1.0)
    middle_across = recentered_aggregates[:, 1] / floored
    middle_along = recentered_aggregates[:, 2] / floored
    along_displacement = along_coordinate - jnp.dot(sweep_membership, middle_along, precision=largest_value)
    across_displacement = across_coordinate[None, :] - jnp.dot(sweep_membership, middle_across, precision=largest_value)[:, None]
    weighted_u = weight * across_displacement
    line_cross_inphase = lax.optimization_barrier(jnp.sum(weight * coh_real, 1))
    line_cross_quadrature = lax.optimization_barrier(jnp.sum(weight * coh_imag, 1))
    along_coordinate_power_two = lax.optimization_barrier(jnp.sum(weighted_u * across_displacement, 1))
    along_first_moment = lax.optimization_barrier(jnp.sum(weighted_u, 1))
    along_weighted_inphase = lax.optimization_barrier(jnp.sum(weighted_u * coh_real, 1))
    along_weighted_quadrature = lax.optimization_barrier(jnp.sum(weighted_u * coh_imag, 1))
    following_picture = sweep_aggregates(sweep_membership, jnp.stack([along_coordinate_power_two, along_displacement * along_first_moment, along_displacement * along_displacement * line_usable_tally, line_cross_inphase, line_cross_quadrature, along_weighted_inphase, along_weighted_quadrature, along_displacement * line_cross_inphase, along_displacement * line_cross_quadrature], 1))
    planar_trends = solve_ramps(pixel_count, following_picture[:, 0], following_picture[:, 1], following_picture[:, 2], following_picture[:, 3:9])
    for_each_line = jnp.dot(sweep_membership, planar_trends, precision=largest_value)
    model_real = for_each_line[:, 0:1] + for_each_line[:, 2:3] * across_displacement + (for_each_line[:, 4] * along_displacement)[:, None]
    model_imag = for_each_line[:, 1:2] + for_each_line[:, 3:4] * across_displacement + (for_each_line[:, 5] * along_displacement)[:, None]
    out_real = coh_real * model_real + coh_imag * model_imag
    out_imag = coh_imag * model_real - coh_real * model_imag
    return (jnp.stack([out_real, out_imag]), coherence)
```

```python
import functools

import jax
import jax.numpy as jnp
from jax import lax
from jax.experimental import pallas as pl
from jax.experimental.pallas import tpu as pltpu
from jax.sharding import PartitionSpec as P

WIN_R = 32
WIN_C = 8
SWEEP_TALLY = 16

EDGE = WIN_R // 2
SIDE = WIN_C // 2
LANES = 128
SCALE = 2.0**56
FLOOR = 1e-36
F32 = jnp.float32
BF16 = jnp.bfloat16
MESH = pl.DeviceIdType.MESH


def masked(av, bv, wv, rows, lanes):
    w = wv[rows, lanes].astype(F32)
    return av[0, rows, lanes] * w, av[1, rows, lanes] * w, bv[0, rows, lanes] * w, bv[1, rows, lanes] * w


def encode(ar, ai, br, bi):
    sr, si = ar * SCALE, ai * SCALE
    power = sr * sr + si * si
    some = power > FLOOR
    inverse = lax.rsqrt(jnp.where(some, power, 1.0))
    return (
        jnp.where(some, power * inverse * (1.0 / SCALE), 0.0),
        jnp.where(some, (sr * br + si * bi) * inverse, br),
        jnp.where(some, (si * br - sr * bi) * inverse, bi),
    )


def decode(s, gr, gi):
    return s * gr, s * gi, s * s, gr * gr + gi * gi


def put_split(out, products, lanes, rows, low_rows):
    for plane, value in enumerate(products):
        high = value.astype(BF16)
        out[plane, rows, lanes] = high
        out[plane, low_rows, lanes] = (value - high.astype(F32)).astype(BF16)


def edge_block(pack):
    lane = lax.broadcasted_iota(jnp.int32, pack.shape, 1)
    left, right = lane >= LANES - SIDE, lane < SIDE

    def pick(k):
        a = pack if k == 0 else pltpu.roll(pack, k * SIDE, 1)
        b = pack if k == 0 else pltpu.roll(pack, LANES - k * SIDE, 1)
        return jnp.where(left, a, jnp.where(right, b, 0.0))

    return pick(0), pick(1), pick(2)


def front_kernel(
    n_rows, n_cols,
    lead, trail, flags, sweep,
    gam, coef, across,
    av, bv, wv, up_out, down_out, top_in, bot_in, left_out, right_out, left_in, right_in,
    corner, corner_top, corner_bot, split, halo_split, vert, lines, member,
    tab_out, tab_cols, sum_out, tab_rows,
    load_sem, halo_send, halo_recv, side_send, side_recv, corner_send, corner_recv,
    cols_send, cols_recv, rows_send, rows_recv,
):
    me_r, me_c = lax.axis_index("rows"), lax.axis_index("cols")
    height, width = flags.shape
    wide = width + LANES
    low = height - EDGE
    chunk = 512 if width % 512 == 0 else LANES
    has_up, has_down = me_r > 0, me_r < n_rows - 1
    has_left, has_right = me_c > 0, me_c < n_cols - 1

    loads = []
    for part, (first, count) in enumerate(((low, EDGE), (0, EDGE), (EDGE, low - EDGE))):
        rows = pl.ds(first, count)
        group = [
            pltpu.make_async_copy(lead.at[:, rows, :], av.at[:, rows, :], load_sem.at[part, 0]),
            pltpu.make_async_copy(trail.at[:, rows, :], bv.at[:, rows, :], load_sem.at[part, 1]),
            pltpu.make_async_copy(flags.at[rows, :], wv.at[rows, :], load_sem.at[part, 2]),
        ]
        for copy in group:
            copy.start()
        loads.append(group)

    barrier = pltpu.get_barrier_semaphore()
    for k in range(1, n_rows):
        pl.semaphore_signal(barrier, inc=1, device_id=(lax.rem(me_r + k, n_rows), me_c), device_id_type=MESH)
    for k in range(1, n_cols):
        pl.semaphore_signal(barrier, inc=1, device_id=(me_r, lax.rem(me_c + k, n_cols)), device_id_type=MESH)

    def remote(src, dst, send, recv, row, col):
        return pltpu.make_async_remote_copy(
            src_ref=src, dst_ref=dst, send_sem=send, recv_sem=recv, device_id=(row, col), device_id_type=MESH
        )

    down = remote(down_out, top_in, halo_send.at[0], halo_recv.at[0], me_r + 1, me_c)
    up = remote(up_out, bot_in, halo_send.at[1], halo_recv.at[1], me_r - 1, me_c)
    to_right = remote(right_out, left_in, side_send.at[0], side_recv.at[0], me_r, me_c + 1)
    to_left = remote(left_out, right_in, side_send.at[1], side_recv.at[1], me_r, me_c - 1)
    corner_down = remote(
        corner.at[pl.ds(low, EDGE)], corner_top, corner_send.at[0], corner_recv.at[0], me_r + 1, me_c
    )
    corner_up = remote(
        corner.at[pl.ds(0, EDGE)], corner_bot, corner_send.at[1], corner_recv.at[1], me_r - 1, me_c
    )

    def encode_rows(first, out):
        @pl.loop(0, width // chunk)
        def _(c):
            lanes = pl.ds(pl.multiple_of(c * chunk, chunk), chunk)
            for k, value in enumerate(encode(*masked(av, bv, wv, pl.ds(first, EDGE), lanes))):
                out[k, :, lanes] = value

    for copy in loads[0]:
        copy.wait()
    encode_rows(low, down_out)
    for copy in loads[1]:
        copy.wait()
    encode_rows(0, up_out)

    pl.semaphore_wait(barrier, n_rows - 1 + n_cols - 1)

    @pl.when(has_down)
    def _():
        down.start()

    @pl.when(has_up)
    def _():
        up.start()

    for copy in loads[2]:
        copy.wait()

    @pl.loop(0, height // 16)
    def _(b):
        rows = pl.ds(pl.multiple_of(b * 16, 16), 16)
        lane = lax.broadcasted_iota(jnp.int32, (16, LANES), 1)
        s, gr, gi = encode(*masked(av, bv, wv, rows, pl.ds(width - LANES, LANES)))
        right_out[rows, :] = jnp.where(
            lane >= LANES - SIDE,
            s,
            jnp.where(
                lane >= LANES - 2 * SIDE,
                pltpu.roll(gr, LANES - SIDE, 1),
                jnp.where(lane >= LANES - 3 * SIDE, pltpu.roll(gi, LANES - 2 * SIDE, 1), 0.0),
            ),
        )
        s, gr, gi = encode(*masked(av, bv, wv, rows, pl.ds(0, LANES)))
        left_out[rows, :] = jnp.where(
            lane < SIDE,
            s,
            jnp.where(
                lane < 2 * SIDE,
                pltpu.roll(gr, SIDE, 1),
                jnp.where(lane < 3 * SIDE, pltpu.roll(gi, 2 * SIDE, 1), 0.0),
            ),
        )

    @pl.when(jnp.logical_not(has_left))
    def _():
        left_in[...] = jnp.zeros_like(left_in)

    @pl.when(jnp.logical_not(has_right))
    def _():
        right_in[...] = jnp.zeros_like(right_in)

    @pl.when(jnp.logical_not(has_up))
    def _():
        top_in[...] = jnp.zeros_like(top_in)
        corner_top[...] = jnp.zeros_like(corner_top)

    @pl.when(jnp.logical_not(has_down))
    def _():
        bot_in[...] = jnp.zeros_like(bot_in)
        corner_bot[...] = jnp.zeros_like(corner_bot)

    @pl.when(has_right)
    def _():
        to_right.start()

    @pl.when(has_left)
    def _():
        to_left.start()

    @pl.loop(0, height // 16)
    def _(b):
        rows = pl.ds(pl.multiple_of(b * 16, 16), 16)
        low_rows = pl.ds(pl.multiple_of(height + b * 16, 16), 16)

        @pl.loop(0, width // chunk)
        def _(c):
            lanes = pl.ds(pl.multiple_of(c * chunk, chunk), chunk)
            ar, ai, br, bi = masked(av, bv, wv, rows, lanes)
            put_split(
                split,
                (ar * br + ai * bi, ai * br - ar * bi, ar * ar + ai * ai, br * br + bi * bi),
                lanes, rows, low_rows,
            )

    total_rows, total_cols = height * n_rows, width * n_cols
    lane_all = lax.broadcasted_iota(jnp.int32, (8, width), 1) + me_c * width
    across[...] = (lane_all.astype(F32) + 0.5) * (2.0 / total_cols) - 1.0
    member[...] = (lax.broadcasted_iota(jnp.int32, (LANES, height), 0) == sweep[...]).astype(F32)

    @pl.when(has_left)
    def _():
        to_right_wait = to_right
        to_right_wait.wait_recv()

    @pl.when(has_right)
    def _():
        to_left.wait_recv()

    @pl.loop(0, height // 16)
    def _(b):
        rows = pl.ds(pl.multiple_of(b * 16, 16), 16)
        low_rows = pl.ds(pl.multiple_of(height + b * 16, 16), 16)
        lane = lax.broadcasted_iota(jnp.int32, (16, LANES), 1)
        pack = jnp.where(lane >= LANES // 2, left_in[rows, :], right_in[rows, :])
        corner[rows, :] = pack
        put_split(split, decode(*edge_block(pack)), pl.ds(width, LANES), rows, low_rows)

    r = lax.broadcasted_iota(jnp.int32, (height, 2 * height), 0)
    k = lax.rem(lax.broadcasted_iota(jnp.int32, (height, 2 * height), 1), height)
    band = jnp.logical_and(k >= r - EDGE, k < r + EDGE).astype(F32).astype(BF16)

    @pl.loop(0, wide // LANES)
    def _(c):
        lanes = pl.ds(pl.multiple_of(c * LANES, LANES), LANES)
        for plane in range(4):
            vert[plane, :, lanes] = jnp.dot(band, split[plane, :, lanes], preferred_element_type=F32)

    @pl.when(has_down)
    def _():
        corner_down.start()

    @pl.when(has_up)
    def _():
        corner_up.start()

    def finish(first):
        rows = pl.ds(first, 8)

        def across_sum(plane):
            x = vert[plane, rows, :]
            x = x + pltpu.roll(x, wide - 1, 1)
            x = x + pltpu.roll(x, wide - 2, 1)
            return x + pltpu.roll(x, wide - 4, 1)

        inverse = lax.rsqrt((across_sum(2) + 1.0) * (across_sum(3) + 1.0))
        real = pltpu.roll(across_sum(0) * inverse, SIDE, 1)[:, :width]
        imag = pltpu.roll(across_sum(1) * inverse, SIDE, 1)[:, :width]
        gam[0, rows, :] = real
        gam[1, rows, :] = imag
        u = across[...]
        w = wv[rows, :].astype(F32)
        wu = w * u
        s0 = jnp.sum(w, 1, keepdims=True)
        su = jnp.sum(wu, 1, keepdims=True)
        suu = jnp.sum(wu * u, 1, keepdims=True)
        hr = jnp.sum(w * real, 1, keepdims=True)
        hi = jnp.sum(w * imag, 1, keepdims=True)
        hur = jnp.sum(wu * real, 1, keepdims=True)
        hui = jnp.sum(wu * imag, 1, keepdims=True)
        row = lax.broadcasted_iota(jnp.int32, (8, 1), 0) + (me_r * height + first)
        v = (row.astype(F32) + 0.5) * (2.0 / total_rows) - 1.0
        lane = lax.broadcasted_iota(jnp.int32, (8, LANES), 1)
        table = jnp.zeros((8, LANES), F32)
        for m, value in enumerate((s0, su, v * s0, suu, v * su, v * v * s0, hr, hi, hur, hui, v * hr, v * hi)):
            table = jnp.where(lane == m, value, table)
        lines[rows, :] = table

    @pl.loop(0, (low - EDGE) // 8)
    def _(b):
        finish(pl.multiple_of(EDGE + b * 8, 8))

    @pl.when(has_up)
    def _():
        down.wait_recv()

    @pl.when(has_down)
    def _():
        up.wait_recv()

    for part, halo in enumerate((top_in, bot_in)):
        rows = pl.ds(2 * part * EDGE, EDGE)
        low_rows = pl.ds((2 * part + 1) * EDGE, EDGE)

        @pl.loop(0, width // chunk)
        def _(c):
            lanes = pl.ds(pl.multiple_of(c * chunk, chunk), chunk)
            put_split(
                halo_split, decode(halo[0, :, lanes], halo[1, :, lanes], halo[2, :, lanes]), lanes, rows, low_rows
            )

    @pl.when(has_up)
    def _():
        corner_down.wait_recv()

    @pl.when(has_down)
    def _():
        corner_up.wait_recv()

    for part, pack in enumerate((corner_top, corner_bot)):
        put_split(
            halo_split, decode(*edge_block(pack[...])), pl.ds(width, LANES),
            pl.ds(2 * part * EDGE, EDGE), pl.ds((2 * part + 1) * EDGE, EDGE),
        )

    r = lax.broadcasted_iota(jnp.int32, (2 * EDGE, 4 * EDGE), 0)
    k = lax.broadcasted_iota(jnp.int32, (2 * EDGE, 4 * EDGE), 1)
    within = lax.rem(k, EDGE)
    upper = jnp.logical_and(jnp.logical_and(r < EDGE, k < 2 * EDGE), within >= r)
    lower = jnp.logical_and(jnp.logical_and(r >= EDGE, k >= 2 * EDGE), within < r - EDGE)
    reach = jnp.logical_or(upper, lower).astype(F32).astype(BF16)

    for plane in range(4):
        extra = jnp.dot(reach, halo_split[plane], preferred_element_type=F32)
        vert[plane, 0:EDGE, :] += extra[:EDGE]
        vert[plane, low:height, :] += extra[EDGE:]

    @pl.loop(0, 2 * EDGE // 8)
    def _(b):
        finish(pl.multiple_of(b * 8 + (b // (EDGE // 8)) * (low - EDGE), 8))

    exact = lax.Precision.HIGHEST
    tab_out[...] = jnp.dot(
        member[0:SWEEP_TALLY, :], lines[...], preferred_element_type=F32, precision=exact
    )
    swaps = [
        remote(tab_out, tab_cols.at[k - 1], cols_send.at[k - 1], cols_recv.at[k - 1], me_r, lax.rem(me_c + k, n_cols))
        for k in range(1, n_cols)
    ]
    for copy in swaps:
        copy.start()
    for copy in swaps:
        copy.wait_recv()
    total = tab_out[...]
    for k in range(n_cols - 1):
        total = total + tab_cols[k]
    sum_out[...] = total
    tours = [
        remote(sum_out, tab_rows.at[k - 1], rows_send.at[k - 1], rows_recv.at[k - 1], lax.rem(me_r + k, n_rows), me_c)
        for k in range(1, n_rows)
    ]
    for copy in tours:
        copy.start()
    for copy in tours:
        copy.wait_recv()
    for k in range(n_rows - 1):
        total = total + tab_rows[k]

    def column(m):
        return total[:, m : m + 1]

    s0, su, sv, suu, suv, svv, hr, hi, hur, hui, hvr, hvi = [column(m) for m in range(12)]
    floored = jnp.maximum(s0, 1.0)
    mid_u, mid_v = su / floored, sv / floored
    guu = suu - 2.0 * mid_u * su + mid_u * mid_u * s0
    guv = suv - mid_u * sv - mid_v * su + mid_u * mid_v * s0
    gvv = svv - 2.0 * mid_v * sv + mid_v * mid_v * s0
    hur, hui = hur - mid_u * hr, hui - mid_u * hi
    hvr, hvi = hvr - mid_v * hr, hvi - mid_v * hi
    ridge = 0.001 * s0 + 1.0
    duu, dvv = guu + ridge, gvv + ridge
    scale = 1.0 / (duu * dvv - guv * guv)
    base = 1.0 / (s0 + ridge)
    fits = (
        mid_u, mid_v, hr * base, hi * base,
        (dvv * hur - guv * hvr) * scale, (dvv * hui - guv * hvi) * scale,
        (duu * hvr - guv * hur) * scale, (duu * hvi - guv * hui) * scale,
    )
    lane = lax.broadcasted_iota(jnp.int32, (SWEEP_TALLY, LANES), 1)
    fit_table = jnp.zeros((SWEEP_TALLY, LANES), F32)
    for m, value in enumerate(fits):
        fit_table = jnp.where(lane == m, value, fit_table)
    spread = jnp.concatenate([fit_table, jnp.zeros((LANES - SWEEP_TALLY, LANES), F32)], 0)
    coef[...] = jnp.dot(member[...].T, spread, preferred_element_type=F32, precision=exact)

    @pl.when(has_down)
    def _():
        down.wait_send()
        corner_down.wait_send()

    @pl.when(has_up)
    def _():
        up.wait_send()
        corner_up.wait_send()

    @pl.when(has_right)
    def _():
        to_right.wait_send()

    @pl.when(has_left)
    def _():
        to_left.wait_send()

    for copy in swaps + tours:
        copy.wait_send()


def back_kernel(n_rows, block, gam, coef, across, ramped, coherence):
    height = gam.shape[1]
    step = pl.program_id(0)
    me_r = lax.axis_index("rows")

    @pl.loop(0, block // 8)
    def _(b):
        inner = pl.ds(pl.multiple_of(b * 8, 8), 8)
        first = pl.multiple_of(step * block + b * 8, 8)
        rows = pl.ds(first, 8)
        line = coef[rows, :]
        row = lax.broadcasted_iota(jnp.int32, (8, 1), 0) + (me_r * height + first)
        v = (row.astype(F32) + 0.5) * (2.0 / (height * n_rows)) - 1.0
        dv = v - line[:, 1:2]
        real, imag = gam[0, rows, :], gam[1, rows, :]
        du = across[...] - line[:, 0:1]
        model_real = (line[:, 2:3] + line[:, 6:7] * dv) + line[:, 4:5] * du
        model_imag = (line[:, 3:4] + line[:, 7:8] * dv) + line[:, 5:6] * du
        ramped[0, inner, :] = real * model_real + imag * model_imag
        ramped[1, inner, :] = imag * model_real - real * model_imag
        coherence[inner, :] = jnp.sqrt(real * real + imag * imag)


def on_device(n_rows, n_cols, lead, trail, flags, sweep):
    height, width = flags.shape
    wide = width + LANES
    any_space = pl.BlockSpec(memory_space=pltpu.HBM)
    vmem = pl.BlockSpec(memory_space=pltpu.VMEM)
    dma = pltpu.SemaphoreType.DMA
    gam, coef, across = pl.pallas_call(
        functools.partial(front_kernel, n_rows, n_cols),
        out_shape=[
            pltpu.VMEM((2, height, width), F32),
            pltpu.VMEM((height, LANES), F32),
            pltpu.VMEM((8, width), F32),
        ],
        in_specs=[any_space, any_space, any_space, vmem],
        out_specs=[vmem, vmem, vmem],
        scratch_shapes=[
            pltpu.VMEM((2, height, width), F32),
            pltpu.VMEM((2, height, width), F32),
            pltpu.VMEM((height, width), jnp.int32),
            pltpu.VMEM((3, EDGE, width), F32),
            pltpu.VMEM((3, EDGE, width), F32),
            pltpu.VMEM((3, EDGE, width), F32),
            pltpu.VMEM((3, EDGE, width), F32),
            pltpu.VMEM((height, LANES), F32),
            pltpu.VMEM((height, LANES), F32),
            pltpu.VMEM((height, LANES), F32),
            pltpu.VMEM((height, LANES), F32),
            pltpu.VMEM((height, LANES), F32),
            pltpu.VMEM((EDGE, LANES), F32),
            pltpu.VMEM((EDGE, LANES), F32),
            pltpu.VMEM((4, 2 * height, wide), BF16),
            pltpu.VMEM((4, 4 * EDGE, wide), BF16),
            pltpu.VMEM((4, height, wide), F32),
            pltpu.VMEM((height, LANES), F32),
            pltpu.VMEM((LANES, height), F32),
            pltpu.VMEM((SWEEP_TALLY, LANES), F32),
            pltpu.VMEM((n_cols - 1, SWEEP_TALLY, LANES), F32),
            pltpu.VMEM((SWEEP_TALLY, LANES), F32),
            pltpu.VMEM((n_rows - 1, SWEEP_TALLY, LANES), F32),
            dma((3, 3)),
            dma((2,)), dma((2,)),
            dma((2,)), dma((2,)),
            dma((2,)), dma((2,)),
            dma((n_cols - 1,)), dma((n_cols - 1,)),
            dma((n_rows - 1,)), dma((n_rows - 1,)),
        ],
        compiler_params=pltpu.CompilerParams(
            collective_id=0, has_side_effects=True, vmem_limit_bytes=40 * 1024 * 1024
        ),
        name="front",
    )(lead, trail, flags, sweep.reshape(1, height))
    block = 32 if height % 32 == 0 else 8
    return pl.pallas_call(
        functools.partial(back_kernel, n_rows, block),
        grid=(height // block,),
        out_shape=[
            jax.ShapeDtypeStruct((2, height, width), F32),
            jax.ShapeDtypeStruct((height, width), F32),
        ],
        in_specs=[vmem, vmem, vmem],
        out_specs=[
            pl.BlockSpec((2, block, width), lambda r: (0, r, 0)),
            pl.BlockSpec((block, width), lambda r: (r, 0)),
        ],
        compiler_params=pltpu.CompilerParams(vmem_limit_bytes=16 * 1024 * 1024),
        name="back",
    )(gam, coef, across)


def solution(mesh):
    return jax.shard_map(
        functools.partial(on_device, mesh.shape["rows"], mesh.shape["cols"]),
        mesh=mesh,
        in_specs=(P(None, "rows", "cols"), P(None, "rows", "cols"), P("rows", "cols"), P("rows")),
        out_specs=(P(None, "rows", "cols"), P("rows", "cols")),
        check_vma=False,
    )
```

```python
import functools

import jax
import jax.numpy as jnp
from jax import lax
from jax.experimental import pallas as pl
from jax.experimental.pallas import tpu as pltpu
from jax.sharding import PartitionSpec as P

WIN_R = 32
WIN_C = 8
SWEEP_TALLY = 16

EDGE = WIN_R // 2
SIDE = WIN_C // 2
LANES = 128
SCALE = 2.0**56
FLOOR = 1e-36
F32 = jnp.float32
BF16 = jnp.bfloat16
MESH = pl.DeviceIdType.MESH


def masked(av, bv, wv, rows, lanes):
    w = wv[rows, lanes].astype(F32)
    return av[0, rows, lanes] * w, av[1, rows, lanes] * w, bv[0, rows, lanes] * w, bv[1, rows, lanes] * w


def encode(ar, ai, br, bi):
    sr, si = ar * SCALE, ai * SCALE
    power = sr * sr + si * si
    some = power > FLOOR
    inverse = lax.rsqrt(jnp.where(some, power, 1.0))
    return (
        jnp.where(some, power * inverse * (1.0 / SCALE), 0.0),
        jnp.where(some, (sr * br + si * bi) * inverse, br),
        jnp.where(some, (si * br - sr * bi) * inverse, bi),
    )


def decode(s, gr, gi):
    return s * gr, s * gi, s * s, gr * gr + gi * gi


def put_split(out, products, lanes, rows, low_rows):
    for plane, value in enumerate(products):
        high = value.astype(BF16)
        out[plane, rows, lanes] = high
        out[plane, low_rows, lanes] = (value - high.astype(F32)).astype(BF16)


def thirds(x):
    high = x.astype(BF16)
    x = x - high.astype(F32)
    middle = x.astype(BF16)
    return [high, middle, (x - middle.astype(F32)).astype(BF16)]


def edge_block(pack):
    lane = lax.broadcasted_iota(jnp.int32, pack.shape, 1)
    left, right = lane >= LANES - SIDE, lane < SIDE

    def pick(k):
        a = pack if k == 0 else pltpu.roll(pack, k * SIDE, 1)
        b = pack if k == 0 else pltpu.roll(pack, LANES - k * SIDE, 1)
        return jnp.where(left, a, jnp.where(right, b, 0.0))

    return pick(0), pick(1), pick(2)


def front_kernel(
    n_rows, n_cols,
    lead, trail, flags, sweep,
    gam, coh, coef, across,
    av, bv, wv, up_out, down_out, top_in, bot_in, left_out, right_out, left_in, right_in,
    corner, corner_top, corner_bot, split, halo_split, vert, lines, member, spread_member, bursts,
    tab_out, tab_cols, sum_out, tab_rows,
    load_sem, halo_send, halo_recv, side_send, side_recv, corner_send, corner_recv,
    cols_send, cols_recv, rows_send, rows_recv,
):
    me_r, me_c = lax.axis_index("rows"), lax.axis_index("cols")
    height, width = flags.shape
    wide = width + LANES
    low = height - EDGE
    chunk = 512 if width % 512 == 0 else LANES
    has_up, has_down = me_r > 0, me_r < n_rows - 1
    has_left, has_right = me_c > 0, me_c < n_cols - 1

    loads = []
    for part, (first, count) in enumerate(((low, EDGE), (0, EDGE), (EDGE, low - EDGE))):
        rows = pl.ds(first, count)
        group = [
            pltpu.make_async_copy(lead.at[:, rows, :], av.at[:, rows, :], load_sem.at[part, 0]),
            pltpu.make_async_copy(trail.at[:, rows, :], bv.at[:, rows, :], load_sem.at[part, 1]),
            pltpu.make_async_copy(flags.at[rows, :], wv.at[rows, :], load_sem.at[part, 2]),
        ]
        for copy in group:
            copy.start()
        loads.append(group)

    burst_load = pltpu.make_async_copy(sweep, bursts, load_sem.at[3, 0])
    burst_load.start()

    barrier = pltpu.get_barrier_semaphore()
    for k in range(1, n_rows):
        pl.semaphore_signal(barrier, inc=1, device_id=(lax.rem(me_r + k, n_rows), me_c), device_id_type=MESH)
    for k in range(1, n_cols):
        pl.semaphore_signal(barrier, inc=1, device_id=(me_r, lax.rem(me_c + k, n_cols)), device_id_type=MESH)

    def remote(src, dst, send, recv, row, col):
        return pltpu.make_async_remote_copy(
            src_ref=src, dst_ref=dst, send_sem=send, recv_sem=recv, device_id=(row, col), device_id_type=MESH
        )

    down = remote(down_out, top_in, halo_send.at[0], halo_recv.at[0], me_r + 1, me_c)
    up = remote(up_out, bot_in, halo_send.at[1], halo_recv.at[1], me_r - 1, me_c)
    to_right = remote(right_out, left_in, side_send.at[0], side_recv.at[0], me_r, me_c + 1)
    to_left = remote(left_out, right_in, side_send.at[1], side_recv.at[1], me_r, me_c - 1)
    corner_down = remote(
        corner.at[pl.ds(low, EDGE)], corner_top, corner_send.at[0], corner_recv.at[0], me_r + 1, me_c
    )
    corner_up = remote(
        corner.at[pl.ds(0, EDGE)], corner_bot, corner_send.at[1], corner_recv.at[1], me_r - 1, me_c
    )

    def encode_rows(first, out):
        @pl.loop(0, width // chunk)
        def _(c):
            lanes = pl.ds(pl.multiple_of(c * chunk, chunk), chunk)
            for k, value in enumerate(encode(*masked(av, bv, wv, pl.ds(first, EDGE), lanes))):
                out[k, :, lanes] = value

    for copy in loads[0]:
        copy.wait()
    encode_rows(low, down_out)
    for copy in loads[1]:
        copy.wait()
    encode_rows(0, up_out)

    pl.semaphore_wait(barrier, n_rows - 1 + n_cols - 1)

    @pl.when(has_down)
    def _():
        down.start()

    for copy in loads[2]:
        copy.wait()

    @pl.loop(0, height // 16)
    def _(b):
        rows = pl.ds(pl.multiple_of(b * 16, 16), 16)
        lane = lax.broadcasted_iota(jnp.int32, (16, LANES), 1)
        s, gr, gi = encode(*masked(av, bv, wv, rows, pl.ds(width - LANES, LANES)))
        right_out[rows, :] = jnp.where(
            lane >= LANES - SIDE,
            s,
            jnp.where(
                lane >= LANES - 2 * SIDE,
                pltpu.roll(gr, LANES - SIDE, 1),
                jnp.where(lane >= LANES - 3 * SIDE, pltpu.roll(gi, LANES - 2 * SIDE, 1), 0.0),
            ),
        )
        s, gr, gi = encode(*masked(av, bv, wv, rows, pl.ds(0, LANES)))
        left_out[rows, :] = jnp.where(
            lane < SIDE,
            s,
            jnp.where(
                lane < 2 * SIDE,
                pltpu.roll(gr, SIDE, 1),
                jnp.where(lane < 3 * SIDE, pltpu.roll(gi, 2 * SIDE, 1), 0.0),
            ),
        )

    @pl.when(jnp.logical_not(has_left))
    def _():
        left_in[...] = jnp.zeros_like(left_in)

    @pl.when(jnp.logical_not(has_right))
    def _():
        right_in[...] = jnp.zeros_like(right_in)

    @pl.when(jnp.logical_not(has_up))
    def _():
        top_in[...] = jnp.zeros_like(top_in)
        corner_top[...] = jnp.zeros_like(corner_top)

    @pl.when(jnp.logical_not(has_down))
    def _():
        bot_in[...] = jnp.zeros_like(bot_in)
        corner_bot[...] = jnp.zeros_like(corner_bot)

    @pl.when(has_right)
    def _():
        to_right.start()

    @pl.when(has_left)
    def _():
        to_left.start()

    @pl.when(has_left)
    def _():
        to_right.wait_recv()

    @pl.when(has_right)
    def _():
        to_left.wait_recv()

    @pl.loop(0, height // 16)
    def _(b):
        rows = pl.ds(pl.multiple_of(b * 16, 16), 16)
        low_rows = pl.ds(pl.multiple_of(height + b * 16, 16), 16)
        lane = lax.broadcasted_iota(jnp.int32, (16, LANES), 1)
        pack = jnp.where(lane >= LANES // 2, left_in[rows, :], right_in[rows, :])
        corner[rows, :] = pack
        put_split(split, decode(*edge_block(pack)), pl.ds(width, LANES), rows, low_rows)

    @pl.when(has_down)
    def _():
        corner_down.start()

    @pl.when(has_up)
    def _():
        up.start()
        corner_up.start()

    @pl.loop(0, height // 16)
    def _(b):
        rows = pl.ds(pl.multiple_of(b * 16, 16), 16)
        low_rows = pl.ds(pl.multiple_of(height + b * 16, 16), 16)

        @pl.loop(0, width // chunk)
        def _(c):
            lanes = pl.ds(pl.multiple_of(c * chunk, chunk), chunk)
            ar, ai, br, bi = masked(av, bv, wv, rows, lanes)
            put_split(
                split,
                (ar * br + ai * bi, ai * br - ar * bi, ar * ar + ai * ai, br * br + bi * bi),
                lanes, rows, low_rows,
            )

    total_rows, total_cols = height * n_rows, width * n_cols
    lane_all = lax.broadcasted_iota(jnp.int32, (8, width), 1) + me_c * width
    across[...] = (lane_all.astype(F32) + 0.5) * (2.0 / total_cols) - 1.0

    burst_load.wait()
    member[...] = (lax.broadcasted_iota(jnp.int32, (SWEEP_TALLY, height), 0) == bursts[...]).astype(BF16)
    third = lax.broadcasted_iota(jnp.int32, (LANES, height), 0)
    third_of = jnp.logical_and(lax.rem(third, SWEEP_TALLY) == bursts[...], third < 3 * SWEEP_TALLY)
    spread_member[...] = third_of.astype(F32).T.astype(BF16)

    r = lax.broadcasted_iota(jnp.int32, (height, 2 * height), 0)
    k = lax.rem(lax.broadcasted_iota(jnp.int32, (height, 2 * height), 1), height)
    band = jnp.logical_and(k >= r - EDGE, k < r + EDGE).astype(F32).astype(BF16)

    @pl.loop(0, wide // LANES)
    def _(c):
        lanes = pl.ds(pl.multiple_of(c * LANES, LANES), LANES)
        for plane in range(4):
            vert[plane, :, lanes] = jnp.dot(band, split[plane, :, lanes], preferred_element_type=F32)

    def finish(first):
        rows = pl.ds(first, 8)

        def across_sum(plane):
            x = vert[plane, rows, :]
            x = x + pltpu.roll(x, wide - 1, 1)
            x = x + pltpu.roll(x, wide - 2, 1)
            return x + pltpu.roll(x, wide - 4, 1)

        inverse = lax.rsqrt((across_sum(2) + 1.0) * (across_sum(3) + 1.0))
        real = pltpu.roll(across_sum(0) * inverse, SIDE, 1)[:, :width]
        imag = pltpu.roll(across_sum(1) * inverse, SIDE, 1)[:, :width]
        gam[0, rows, :] = real
        gam[1, rows, :] = imag
        coh[rows, :] = jnp.sqrt(real * real + imag * imag)
        u = across[...]
        w = wv[rows, :].astype(F32)
        wu = w * u
        s0 = jnp.sum(w, 1, keepdims=True)
        su = jnp.sum(wu, 1, keepdims=True)
        suu = jnp.sum(wu * u, 1, keepdims=True)
        hr = jnp.sum(w * real, 1, keepdims=True)
        hi = jnp.sum(w * imag, 1, keepdims=True)
        hur = jnp.sum(wu * real, 1, keepdims=True)
        hui = jnp.sum(wu * imag, 1, keepdims=True)
        row = lax.broadcasted_iota(jnp.int32, (8, 1), 0) + (me_r * height + first)
        v = (row.astype(F32) + 0.5) * (2.0 / total_rows) - 1.0
        lane = lax.broadcasted_iota(jnp.int32, (8, LANES), 1)
        table = jnp.zeros((8, LANES), F32)
        for m, value in enumerate((s0, su, v * s0, suu, v * su, v * v * s0, hr, hi, hur, hui, v * hr, v * hi)):
            table = jnp.where(lane == m, value, table)
        lines[rows, :] = table

    @pl.loop(0, (low - EDGE) // 8)
    def _(b):
        finish(pl.multiple_of(EDGE + b * 8, 8))

    r = lax.broadcasted_iota(jnp.int32, (EDGE, 2 * EDGE), 0)
    k = lax.rem(lax.broadcasted_iota(jnp.int32, (EDGE, 2 * EDGE), 1), EDGE)
    reaches = ((k >= r).astype(F32).astype(BF16), (k < r).astype(F32).astype(BF16))
    sides = (
        (has_up, down, corner_down, top_in, corner_top, 0),
        (has_down, up, corner_up, bot_in, corner_bot, low),
    )
    for part, (there, main, extra_copy, halo, pack, first) in enumerate(sides):

        @pl.when(there)
        def _():
            main.wait_recv()

        rows = pl.ds(2 * part * EDGE, EDGE)
        low_rows = pl.ds((2 * part + 1) * EDGE, EDGE)

        @pl.loop(0, width // chunk)
        def _(c):
            lanes = pl.ds(pl.multiple_of(c * chunk, chunk), chunk)
            put_split(
                halo_split, decode(halo[0, :, lanes], halo[1, :, lanes], halo[2, :, lanes]), lanes, rows, low_rows
            )

        @pl.when(there)
        def _():
            extra_copy.wait_recv()

        put_split(halo_split, decode(*edge_block(pack[...])), pl.ds(width, LANES), rows, low_rows)
        for plane in range(4):
            vert[plane, first : first + EDGE, :] += jnp.dot(
                reaches[part], halo_split[plane, pl.ds(2 * part * EDGE, 2 * EDGE), :], preferred_element_type=F32
            )

        @pl.loop(0, EDGE // 8)
        def _(b):
            finish(pl.multiple_of(first + b * 8, 8))

    tab_out[...] = jnp.dot(
        jnp.concatenate([member[...]] * 3, 1),
        jnp.concatenate(thirds(lines[...]), 0),
        preferred_element_type=F32,
    )
    swaps = [
        remote(tab_out, tab_cols.at[k - 1], cols_send.at[k - 1], cols_recv.at[k - 1], me_r, lax.rem(me_c + k, n_cols))
        for k in range(1, n_cols)
    ]
    for copy in swaps:
        copy.start()
    for copy in swaps:
        copy.wait_recv()
    total = tab_out[...]
    for k in range(n_cols - 1):
        total = total + tab_cols[k]
    sum_out[...] = total
    tours = [
        remote(sum_out, tab_rows.at[k - 1], rows_send.at[k - 1], rows_recv.at[k - 1], lax.rem(me_r + k, n_rows), me_c)
        for k in range(1, n_rows)
    ]
    for copy in tours:
        copy.start()
    for copy in tours:
        copy.wait_recv()
    for k in range(n_rows - 1):
        total = total + tab_rows[k]

    def column(m):
        return total[:, m : m + 1]

    s0, su, sv, suu, suv, svv, hr, hi, hur, hui, hvr, hvi = [column(m) for m in range(12)]
    floored = jnp.maximum(s0, 1.0)
    mid_u, mid_v = su / floored, sv / floored
    guu = suu - 2.0 * mid_u * su + mid_u * mid_u * s0
    guv = suv - mid_u * sv - mid_v * su + mid_u * mid_v * s0
    gvv = svv - 2.0 * mid_v * sv + mid_v * mid_v * s0
    hur, hui = hur - mid_u * hr, hui - mid_u * hi
    hvr, hvi = hvr - mid_v * hr, hvi - mid_v * hi
    ridge = 0.001 * s0 + 1.0
    duu, dvv = guu + ridge, gvv + ridge
    scale = 1.0 / (duu * dvv - guv * guv)
    base = 1.0 / (s0 + ridge)
    fits = (
        mid_u, mid_v, hr * base, hi * base,
        (dvv * hur - guv * hvr) * scale, (dvv * hui - guv * hvi) * scale,
        (duu * hvr - guv * hur) * scale, (duu * hvi - guv * hui) * scale,
    )
    lane = lax.broadcasted_iota(jnp.int32, (SWEEP_TALLY, LANES), 1)
    fit_table = jnp.zeros((SWEEP_TALLY, LANES), F32)
    for m, value in enumerate(fits):
        fit_table = jnp.where(lane == m, value, fit_table)
    rest = jnp.zeros((LANES - 3 * SWEEP_TALLY, LANES), BF16)
    coef[...] = jnp.dot(
        spread_member[...], jnp.concatenate(thirds(fit_table) + [rest], 0), preferred_element_type=F32
    )

    @pl.when(has_down)
    def _():
        down.wait_send()
        corner_down.wait_send()

    @pl.when(has_up)
    def _():
        up.wait_send()
        corner_up.wait_send()

    @pl.when(has_right)
    def _():
        to_right.wait_send()

    @pl.when(has_left)
    def _():
        to_left.wait_send()

    for copy in swaps + tours:
        copy.wait_send()


def back_kernel(n_rows, block, gam, coh, coef, across, ramped, coherence, out, sems):
    height = gam.shape[1]
    me_r = lax.axis_index("rows")
    whole = pltpu.make_async_copy(coh, coherence, sems.at[height // block])
    whole.start()
    copies = []
    for step in range(height // block):
        for first in range(step * block, (step + 1) * block, 8):
            rows = pl.ds(first, 8)
            line = coef[rows, :]
            row = lax.broadcasted_iota(jnp.int32, (8, 1), 0) + (me_r * height + first)
            v = (row.astype(F32) + 0.5) * (2.0 / (height * n_rows)) - 1.0
            dv = v - line[:, 1:2]
            real, imag = gam[0, rows, :], gam[1, rows, :]
            du = across[...] - line[:, 0:1]
            model_real = (line[:, 2:3] + line[:, 6:7] * dv) + line[:, 4:5] * du
            model_imag = (line[:, 3:4] + line[:, 7:8] * dv) + line[:, 5:6] * du
            out[0, rows, :] = real * model_real + imag * model_imag
            out[1, rows, :] = imag * model_real - real * model_imag
        rows = pl.ds(step * block, block)
        copy = pltpu.make_async_copy(out.at[:, rows, :], ramped.at[:, rows, :], sems.at[step])
        copy.start()
        copies.append(copy)
    for copy in copies:
        copy.wait()
    whole.wait()


def on_device(n_rows, n_cols, lead, trail, flags, sweep):
    height, width = flags.shape
    wide = width + LANES
    any_space = pl.BlockSpec(memory_space=pltpu.HBM)
    vmem = pl.BlockSpec(memory_space=pltpu.VMEM)
    dma = pltpu.SemaphoreType.DMA
    gam, coh, coef, across = pl.pallas_call(
        functools.partial(front_kernel, n_rows, n_cols),
        out_shape=[
            pltpu.VMEM((2, height, width), F32),
            pltpu.VMEM((height, width), F32),
            pltpu.VMEM((height, LANES), F32),
            pltpu.VMEM((8, width), F32),
        ],
        in_specs=[any_space] * 4,
        out_specs=[vmem] * 4,
        scratch_shapes=[
            pltpu.VMEM((2, height, width), F32),
            pltpu.VMEM((2, height, width), F32),
            pltpu.VMEM((height, width), jnp.int32),
            pltpu.VMEM((3, EDGE, width), F32),
            pltpu.VMEM((3, EDGE, width), F32),
            pltpu.VMEM((3, EDGE, width), F32),
            pltpu.VMEM((3, EDGE, width), F32),
            pltpu.VMEM((height, LANES), F32),
            pltpu.VMEM((height, LANES), F32),
            pltpu.VMEM((height, LANES), F32),
            pltpu.VMEM((height, LANES), F32),
            pltpu.VMEM((height, LANES), F32),
            pltpu.VMEM((EDGE, LANES), F32),
            pltpu.VMEM((EDGE, LANES), F32),
            pltpu.VMEM((4, 2 * height, wide), BF16),
            pltpu.VMEM((4, 4 * EDGE, wide), BF16),
            pltpu.VMEM((4, height, wide), F32),
            pltpu.VMEM((height, LANES), F32),
            pltpu.VMEM((SWEEP_TALLY, height), BF16),
            pltpu.VMEM((height, LANES), BF16),
            pltpu.VMEM((1, height), jnp.int32),
            pltpu.VMEM((SWEEP_TALLY, LANES), F32),
            pltpu.VMEM((n_cols - 1, SWEEP_TALLY, LANES), F32),
            pltpu.VMEM((SWEEP_TALLY, LANES), F32),
            pltpu.VMEM((n_rows - 1, SWEEP_TALLY, LANES), F32),
            dma((4, 3)),
            dma((2,)), dma((2,)),
            dma((2,)), dma((2,)),
            dma((2,)), dma((2,)),
            dma((n_cols - 1,)), dma((n_cols - 1,)),
            dma((n_rows - 1,)), dma((n_rows - 1,)),
        ],
        compiler_params=pltpu.CompilerParams(
            collective_id=0, has_side_effects=True, vmem_limit_bytes=40 * 1024 * 1024
        ),
        name="front",
    )(*(pltpu.with_memory_space_constraint(x, pltpu.HBM) for x in (lead, trail, flags, sweep.reshape(1, height))))
    block = 32 if height % 32 == 0 else 8
    return pl.pallas_call(
        functools.partial(back_kernel, n_rows, block),
        out_shape=[
            jax.ShapeDtypeStruct((2, height, width), F32),
            jax.ShapeDtypeStruct((height, width), F32),
        ],
        in_specs=[vmem] * 4,
        out_specs=[any_space, any_space],
        scratch_shapes=[pltpu.VMEM((2, height, width), F32), dma((height // block + 1,))],
        compiler_params=pltpu.CompilerParams(vmem_limit_bytes=16 * 1024 * 1024),
        name="back",
    )(gam, coh, coef, across)


def solution(mesh):
    return jax.shard_map(
        functools.partial(on_device, mesh.shape["rows"], mesh.shape["cols"]),
        mesh=mesh,
        in_specs=(P(None, "rows", "cols"), P(None, "rows", "cols"), P("rows", "cols"), P("rows")),
        out_specs=(P(None, "rows", "cols"), P("rows", "cols")),
        check_vma=False,
    )
```

```python
import functools

import jax
import jax.numpy as jnp
from jax import lax
from jax.experimental import pallas as pl
from jax.experimental.pallas import tpu as pltpu
from jax.sharding import PartitionSpec as P

WIN_R = 32
WIN_C = 8
SWEEP_TALLY = 16

EDGE = WIN_R // 2
SIDE = WIN_C // 2
LANES = 128
GROUP = LANES // SWEEP_TALLY
SCALE = 2.0**56
FLOOR = 1e-36
F32 = jnp.float32
BF16 = jnp.bfloat16
MESH = pl.DeviceIdType.MESH


def masked(av, bv, wv, rows, lanes):
    w = wv[rows, lanes].astype(F32)
    return av[0, rows, lanes] * w, av[1, rows, lanes] * w, bv[0, rows, lanes] * w, bv[1, rows, lanes] * w


def encode(ar, ai, br, bi):
    sr, si = ar * SCALE, ai * SCALE
    power = sr * sr + si * si
    some = power > FLOOR
    inverse = lax.rsqrt(jnp.where(some, power, 1.0))
    return (
        jnp.where(some, power * inverse * (1.0 / SCALE), 0.0),
        jnp.where(some, (sr * br + si * bi) * inverse, br),
        jnp.where(some, (si * br - sr * bi) * inverse, bi),
    )


def decode(s, gr, gi):
    return s * gr, s * gi, s * s, gr * gr + gi * gi


def put_split(out, products, lanes, rows, low_rows):
    for plane, value in enumerate(products):
        high = value.astype(BF16)
        out[plane, rows, lanes] = high
        out[plane, low_rows, lanes] = (value - high.astype(F32)).astype(BF16)


def edge_block(pack):
    lane = lax.broadcasted_iota(jnp.int32, pack.shape, 1)
    left, right = lane >= LANES - SIDE, lane < SIDE

    def pick(k):
        a = pack if k == 0 else pltpu.roll(pack, k * SIDE, 1)
        b = pack if k == 0 else pltpu.roll(pack, LANES - k * SIDE, 1)
        return jnp.where(left, a, jnp.where(right, b, 0.0))

    return pick(0), pick(1), pick(2)


def front_kernel(
    n_rows, n_cols,
    lead, trail, flags, sweep,
    gam, coh, coef, across,
    av, bv, wv, up_out, down_out, top_in, bot_in, left_out, right_out, left_in, right_in,
    corner, corner_top, corner_bot, split, halo_split, vert, lines, member, bursts,
    tab_out, tab_cols, sum_out, tab_rows,
    load_sem, halo_send, halo_recv, side_send, side_recv, corner_send, corner_recv,
    cols_send, cols_recv, rows_send, rows_recv,
):
    me_r, me_c = lax.axis_index("rows"), lax.axis_index("cols")
    height, width = flags.shape
    wide = width + LANES
    low = height - EDGE
    chunk = 512 if width % 512 == 0 else LANES
    has_up, has_down = me_r > 0, me_r < n_rows - 1
    has_left, has_right = me_c > 0, me_c < n_cols - 1

    loads = []
    for part, (first, count) in enumerate(((low, EDGE), (0, EDGE), (EDGE, low - EDGE))):
        rows = pl.ds(first, count)
        group = [
            pltpu.make_async_copy(lead.at[:, rows, :], av.at[:, rows, :], load_sem.at[part, 0]),
            pltpu.make_async_copy(trail.at[:, rows, :], bv.at[:, rows, :], load_sem.at[part, 1]),
            pltpu.make_async_copy(flags.at[rows, :], wv.at[rows, :], load_sem.at[part, 2]),
        ]
        for copy in group:
            copy.start()
        loads.append(group)

    burst_load = pltpu.make_async_copy(sweep, bursts, load_sem.at[3, 0])
    burst_load.start()

    barrier = pltpu.get_barrier_semaphore()
    for k in range(1, n_rows):
        pl.semaphore_signal(barrier, inc=1, device_id=(lax.rem(me_r + k, n_rows), me_c), device_id_type=MESH)
    for k in range(1, n_cols):
        pl.semaphore_signal(barrier, inc=1, device_id=(me_r, lax.rem(me_c + k, n_cols)), device_id_type=MESH)

    def remote(src, dst, send, recv, row, col):
        return pltpu.make_async_remote_copy(
            src_ref=src, dst_ref=dst, send_sem=send, recv_sem=recv, device_id=(row, col), device_id_type=MESH
        )

    down = remote(down_out, top_in, halo_send.at[0], halo_recv.at[0], me_r + 1, me_c)
    up = remote(up_out, bot_in, halo_send.at[1], halo_recv.at[1], me_r - 1, me_c)
    to_right = remote(right_out, left_in, side_send.at[0], side_recv.at[0], me_r, me_c + 1)
    to_left = remote(left_out, right_in, side_send.at[1], side_recv.at[1], me_r, me_c - 1)
    corner_down = remote(
        corner.at[pl.ds(low, EDGE)], corner_top, corner_send.at[0], corner_recv.at[0], me_r + 1, me_c
    )
    corner_up = remote(
        corner.at[pl.ds(0, EDGE)], corner_bot, corner_send.at[1], corner_recv.at[1], me_r - 1, me_c
    )

    def encode_rows(first, out):
        @pl.loop(0, width // chunk)
        def _(c):
            lanes = pl.ds(pl.multiple_of(c * chunk, chunk), chunk)
            for k, value in enumerate(encode(*masked(av, bv, wv, pl.ds(first, EDGE), lanes))):
                out[k, :, lanes] = value

    for copy in loads[0]:
        copy.wait()
    encode_rows(low, down_out)
    for copy in loads[1]:
        copy.wait()
    encode_rows(0, up_out)

    pl.semaphore_wait(barrier, n_rows - 1 + n_cols - 1)

    @pl.when(has_down)
    def _():
        down.start()

    for copy in loads[2]:
        copy.wait()

    @pl.loop(0, height // 16)
    def _(b):
        rows = pl.ds(pl.multiple_of(b * 16, 16), 16)
        lane = lax.broadcasted_iota(jnp.int32, (16, LANES), 1)
        s, gr, gi = encode(*masked(av, bv, wv, rows, pl.ds(width - LANES, LANES)))
        right_out[rows, :] = jnp.where(
            lane >= LANES - SIDE,
            s,
            jnp.where(
                lane >= LANES - 2 * SIDE,
                pltpu.roll(gr, LANES - SIDE, 1),
                jnp.where(lane >= LANES - 3 * SIDE, pltpu.roll(gi, LANES - 2 * SIDE, 1), 0.0),
            ),
        )
        s, gr, gi = encode(*masked(av, bv, wv, rows, pl.ds(0, LANES)))
        left_out[rows, :] = jnp.where(
            lane < SIDE,
            s,
            jnp.where(
                lane < 2 * SIDE,
                pltpu.roll(gr, SIDE, 1),
                jnp.where(lane < 3 * SIDE, pltpu.roll(gi, 2 * SIDE, 1), 0.0),
            ),
        )

    @pl.when(jnp.logical_not(has_left))
    def _():
        left_in[...] = jnp.zeros_like(left_in)

    @pl.when(jnp.logical_not(has_right))
    def _():
        right_in[...] = jnp.zeros_like(right_in)

    @pl.when(jnp.logical_not(has_up))
    def _():
        top_in[...] = jnp.zeros_like(top_in)
        corner_top[...] = jnp.zeros_like(corner_top)

    @pl.when(jnp.logical_not(has_down))
    def _():
        bot_in[...] = jnp.zeros_like(bot_in)
        corner_bot[...] = jnp.zeros_like(corner_bot)

    @pl.when(has_right)
    def _():
        to_right.start()

    @pl.when(has_left)
    def _():
        to_left.start()

    @pl.when(has_left)
    def _():
        to_right.wait_recv()

    @pl.when(has_right)
    def _():
        to_left.wait_recv()

    @pl.loop(0, height // 16)
    def _(b):
        rows = pl.ds(pl.multiple_of(b * 16, 16), 16)
        low_rows = pl.ds(pl.multiple_of(height + b * 16, 16), 16)
        lane = lax.broadcasted_iota(jnp.int32, (16, LANES), 1)
        pack = jnp.where(lane >= LANES // 2, left_in[rows, :], right_in[rows, :])
        corner[rows, :] = pack
        put_split(split, decode(*edge_block(pack)), pl.ds(width, LANES), rows, low_rows)

    @pl.when(has_down)
    def _():
        corner_down.start()

    @pl.when(has_up)
    def _():
        up.start()
        corner_up.start()

    @pl.loop(0, height // 16)
    def _(b):
        rows = pl.ds(pl.multiple_of(b * 16, 16), 16)
        low_rows = pl.ds(pl.multiple_of(height + b * 16, 16), 16)

        @pl.loop(0, width // chunk)
        def _(c):
            lanes = pl.ds(pl.multiple_of(c * chunk, chunk), chunk)
            ar, ai, br, bi = masked(av, bv, wv, rows, lanes)
            put_split(
                split,
                (ar * br + ai * bi, ai * br - ar * bi, ar * ar + ai * ai, br * br + bi * bi),
                lanes, rows, low_rows,
            )

    total_rows, total_cols = height * n_rows, width * n_cols
    lane_all = lax.broadcasted_iota(jnp.int32, (8, width), 1) + me_c * width
    across[...] = (lane_all.astype(F32) + 0.5) * (2.0 / total_cols) - 1.0

    burst_load.wait()
    group_lane = lax.broadcasted_iota(jnp.int32, (LANES, height), 0) // GROUP
    member[...] = (group_lane == bursts[...]).astype(F32).T

    r = lax.broadcasted_iota(jnp.int32, (height, 2 * height), 0)
    k = lax.rem(lax.broadcasted_iota(jnp.int32, (height, 2 * height), 1), height)
    band = jnp.logical_and(k >= r - EDGE, k < r + EDGE).astype(F32).astype(BF16)

    @pl.loop(0, wide // LANES)
    def _(c):
        lanes = pl.ds(pl.multiple_of(c * LANES, LANES), LANES)
        for plane in range(4):
            vert[plane, :, lanes] = jnp.dot(band, split[plane, :, lanes], preferred_element_type=F32)

    def finish(first):
        rows = pl.ds(first, 8)

        def across_sum(plane):
            x = vert[plane, rows, :]
            x = x + pltpu.roll(x, wide - 1, 1)
            x = x + pltpu.roll(x, wide - 2, 1)
            return x + pltpu.roll(x, wide - 4, 1)

        inverse = lax.rsqrt((across_sum(2) + 1.0) * (across_sum(3) + 1.0))
        real = pltpu.roll(across_sum(0) * inverse, SIDE, 1)[:, :width]
        imag = pltpu.roll(across_sum(1) * inverse, SIDE, 1)[:, :width]
        gam[0, rows, :] = real
        gam[1, rows, :] = imag
        coh[rows, :] = jnp.sqrt(real * real + imag * imag)
        u = across[...]
        w = wv[rows, :].astype(F32)
        wu = w * u
        s0 = jnp.sum(w, 1, keepdims=True)
        su = jnp.sum(wu, 1, keepdims=True)
        suu = jnp.sum(wu * u, 1, keepdims=True)
        hr = jnp.sum(w * real, 1, keepdims=True)
        hi = jnp.sum(w * imag, 1, keepdims=True)
        hur = jnp.sum(wu * real, 1, keepdims=True)
        hui = jnp.sum(wu * imag, 1, keepdims=True)
        row = lax.broadcasted_iota(jnp.int32, (8, 1), 0) + (me_r * height + first)
        v = (row.astype(F32) + 0.5) * (2.0 / total_rows) - 1.0
        within = lax.rem(lax.broadcasted_iota(jnp.int32, (8, LANES), 1), GROUP)
        values = (s0, su, v * s0, suu, v * su, v * v * s0, hr, hi, hur, hui, v * hr, v * hi)
        for half in range(2):
            table = jnp.zeros((8, LANES), F32)
            for m, value in enumerate(values[half * GROUP : (half + 1) * GROUP]):
                table = jnp.where(within == m, value, table)
            lines[half, rows, :] = table

    @pl.loop(0, (low - EDGE) // 8, unroll=2)
    def _(b):
        finish(pl.multiple_of(EDGE + b * 8, 8))

    r = lax.broadcasted_iota(jnp.int32, (EDGE, 2 * EDGE), 0)
    k = lax.rem(lax.broadcasted_iota(jnp.int32, (EDGE, 2 * EDGE), 1), EDGE)
    reaches = ((k >= r).astype(F32).astype(BF16), (k < r).astype(F32).astype(BF16))
    sides = (
        (has_up, down, corner_down, top_in, corner_top, 0),
        (has_down, up, corner_up, bot_in, corner_bot, low),
    )
    for part, (there, main, extra_copy, halo, pack, first) in enumerate(sides):

        @pl.when(there)
        def _():
            main.wait_recv()

        rows = pl.ds(2 * part * EDGE, EDGE)
        low_rows = pl.ds((2 * part + 1) * EDGE, EDGE)

        @pl.loop(0, width // chunk)
        def _(c):
            lanes = pl.ds(pl.multiple_of(c * chunk, chunk), chunk)
            put_split(
                halo_split, decode(halo[0, :, lanes], halo[1, :, lanes], halo[2, :, lanes]), lanes, rows, low_rows
            )

        @pl.when(there)
        def _():
            extra_copy.wait_recv()

        put_split(halo_split, decode(*edge_block(pack[...])), pl.ds(width, LANES), rows, low_rows)
        for plane in range(4):
            vert[plane, first : first + EDGE, :] += jnp.dot(
                reaches[part], halo_split[plane, pl.ds(2 * part * EDGE, 2 * EDGE), :], preferred_element_type=F32
            )

        @pl.loop(0, EDGE // 8, unroll=True)
        def _(b):
            finish(pl.multiple_of(first + b * 8, 8))

    mine = member[...] > 0.5
    for half in range(2):
        tab_out[half : half + 1, :] = jnp.sum(jnp.where(mine, lines[half], 0.0), 0, keepdims=True)
    swaps = [
        remote(tab_out, tab_cols.at[k - 1], cols_send.at[k - 1], cols_recv.at[k - 1], me_r, lax.rem(me_c + k, n_cols))
        for k in range(1, n_cols)
    ]
    for copy in swaps:
        copy.start()
    for copy in swaps:
        copy.wait_recv()
    total = tab_out[...]
    for k in range(n_cols - 1):
        total = total + tab_cols[k]
    sum_out[...] = total
    tours = [
        remote(sum_out, tab_rows.at[k - 1], rows_send.at[k - 1], rows_recv.at[k - 1], lax.rem(me_r + k, n_rows), me_c)
        for k in range(1, n_rows)
    ]
    for copy in tours:
        copy.start()
    for copy in tours:
        copy.wait_recv()
    for k in range(n_rows - 1):
        total = total + tab_rows[k]

    def column(m):
        part = total[m // GROUP : m // GROUP + 1, :]
        return part if m % GROUP == 0 else pltpu.roll(part, LANES - m % GROUP, 1)

    s0, su, sv, suu, suv, svv, hr, hi, hur, hui, hvr, hvi = [column(m) for m in range(12)]
    floored = jnp.maximum(s0, 1.0)
    mid_u, mid_v = su / floored, sv / floored
    guu = suu - 2.0 * mid_u * su + mid_u * mid_u * s0
    guv = suv - mid_u * sv - mid_v * su + mid_u * mid_v * s0
    gvv = svv - 2.0 * mid_v * sv + mid_v * mid_v * s0
    hur, hui = hur - mid_u * hr, hui - mid_u * hi
    hvr, hvi = hvr - mid_v * hr, hvi - mid_v * hi
    ridge = 0.001 * s0 + 1.0
    duu, dvv = guu + ridge, gvv + ridge
    scale = 1.0 / (duu * dvv - guv * guv)
    base = 1.0 / (s0 + ridge)
    fits = (
        mid_u, mid_v, hr * base, hi * base,
        (dvv * hur - guv * hvr) * scale, (dvv * hui - guv * hvi) * scale,
        (duu * hvr - guv * hur) * scale, (duu * hvi - guv * hui) * scale,
    )
    within = lax.rem(lax.broadcasted_iota(jnp.int32, (1, LANES), 1), GROUP)
    fit_table = jnp.zeros((1, LANES), F32)
    for m, value in enumerate(fits):
        fit_table = jnp.where(within == m, value if m == 0 else pltpu.roll(value, m, 1), fit_table)
    folded = jnp.where(mine, fit_table, 0.0)
    reach = LANES // 2
    while reach >= GROUP:
        folded = folded + pltpu.roll(folded, reach, 1)
        reach //= 2
    coef[...] = folded

    @pl.when(has_down)
    def _():
        down.wait_send()
        corner_down.wait_send()

    @pl.when(has_up)
    def _():
        up.wait_send()
        corner_up.wait_send()

    @pl.when(has_right)
    def _():
        to_right.wait_send()

    @pl.when(has_left)
    def _():
        to_left.wait_send()

    for copy in swaps + tours:
        copy.wait_send()


def back_kernel(n_rows, block, gam, coh, coef, across, ramped, coherence, out, sems):
    height = gam.shape[1]
    me_r = lax.axis_index("rows")
    whole = pltpu.make_async_copy(coh, coherence, sems.at[height // block])
    whole.start()
    copies = []
    for step in range(height // block):
        for first in range(step * block, (step + 1) * block, 8):
            rows = pl.ds(first, 8)
            line = coef[rows, :]
            row = lax.broadcasted_iota(jnp.int32, (8, 1), 0) + (me_r * height + first)
            v = (row.astype(F32) + 0.5) * (2.0 / (height * n_rows)) - 1.0
            dv = v - line[:, 1:2]
            real, imag = gam[0, rows, :], gam[1, rows, :]
            du = across[...] - line[:, 0:1]
            model_real = (line[:, 2:3] + line[:, 6:7] * dv) + line[:, 4:5] * du
            model_imag = (line[:, 3:4] + line[:, 7:8] * dv) + line[:, 5:6] * du
            out[0, rows, :] = real * model_real + imag * model_imag
            out[1, rows, :] = imag * model_real - real * model_imag
        rows = pl.ds(step * block, block)
        copy = pltpu.make_async_copy(out.at[:, rows, :], ramped.at[:, rows, :], sems.at[step])
        copy.start()
        copies.append(copy)
    for copy in copies:
        copy.wait()
    whole.wait()


def on_device(n_rows, n_cols, lead, trail, flags, sweep):
    height, width = flags.shape
    wide = width + LANES
    any_space = pl.BlockSpec(memory_space=pltpu.HBM)
    vmem = pl.BlockSpec(memory_space=pltpu.VMEM)
    dma = pltpu.SemaphoreType.DMA
    gam, coh, coef, across = pl.pallas_call(
        functools.partial(front_kernel, n_rows, n_cols),
        out_shape=[
            pltpu.VMEM((2, height, width), F32),
            pltpu.VMEM((height, width), F32),
            pltpu.VMEM((height, LANES), F32),
            pltpu.VMEM((8, width), F32),
        ],
        in_specs=[any_space] * 4,
        out_specs=[vmem] * 4,
        scratch_shapes=[
            pltpu.VMEM((2, height, width), F32),
            pltpu.VMEM((2, height, width), F32),
            pltpu.VMEM((height, width), jnp.int32),
            pltpu.VMEM((3, EDGE, width), F32),
            pltpu.VMEM((3, EDGE, width), F32),
            pltpu.VMEM((3, EDGE, width), F32),
            pltpu.VMEM((3, EDGE, width), F32),
            pltpu.VMEM((height, LANES), F32),
            pltpu.VMEM((height, LANES), F32),
            pltpu.VMEM((height, LANES), F32),
            pltpu.VMEM((height, LANES), F32),
            pltpu.VMEM((height, LANES), F32),
            pltpu.VMEM((EDGE, LANES), F32),
            pltpu.VMEM((EDGE, LANES), F32),
            pltpu.VMEM((4, 2 * height, wide), BF16),
            pltpu.VMEM((4, 4 * EDGE, wide), BF16),
            pltpu.VMEM((4, height, wide), F32),
            pltpu.VMEM((2, height, LANES), F32),
            pltpu.VMEM((height, LANES), F32),
            pltpu.VMEM((1, height), jnp.int32),
            pltpu.VMEM((2, LANES), F32),
            pltpu.VMEM((n_cols - 1, 2, LANES), F32),
            pltpu.VMEM((2, LANES), F32),
            pltpu.VMEM((n_rows - 1, 2, LANES), F32),
            dma((4, 3)),
            dma((2,)), dma((2,)),
            dma((2,)), dma((2,)),
            dma((2,)), dma((2,)),
            dma((n_cols - 1,)), dma((n_cols - 1,)),
            dma((n_rows - 1,)), dma((n_rows - 1,)),
        ],
        compiler_params=pltpu.CompilerParams(
            collective_id=0, has_side_effects=True, vmem_limit_bytes=40 * 1024 * 1024
        ),
        name="front",
    )(*(pltpu.with_memory_space_constraint(x, pltpu.HBM) for x in (lead, trail, flags, sweep.reshape(1, height))))
    block = 32 if height % 32 == 0 else 8
    return pl.pallas_call(
        functools.partial(back_kernel, n_rows, block),
        out_shape=[
            jax.ShapeDtypeStruct((2, height, width), F32),
            jax.ShapeDtypeStruct((height, width), F32),
        ],
        in_specs=[vmem] * 4,
        out_specs=[any_space, any_space],
        scratch_shapes=[pltpu.VMEM((2, height, width), F32), dma((height // block + 1,))],
        compiler_params=pltpu.CompilerParams(vmem_limit_bytes=16 * 1024 * 1024),
        name="back",
    )(gam, coh, coef, across)


def solution(mesh):
    return jax.shard_map(
        functools.partial(on_device, mesh.shape["rows"], mesh.shape["cols"]),
        mesh=mesh,
        in_specs=(P(None, "rows", "cols"), P(None, "rows", "cols"), P("rows", "cols"), P("rows")),
        out_specs=(P(None, "rows", "cols"), P("rows", "cols")),
        check_vma=False,
    )
```
